32 devices in a mesh: seq: 8 (over z, x), tp: 4 (over y, core).
Axes of the slice: x: 2, y: 2, z: 4, core: 2. Of those that a mesh axis runs over, the one named last changes fastest.
Arguments:
- inputs: bfloat16 [2, 2048, 2048], P(None, 'seq'), may hold values from -6 to 6
- cotangent: bfloat16 [2, 2048, 2048], P(None, 'seq'), may hold values from -6 to 6
- attn_gain: bfloat16 [2048], P('seq'), may hold values from 0.5 to 1.5
- w_query: bfloat16 [2048, 2048], P('seq', 'tp'), may hold values from -0.125 to 0.125
- w_key: bfloat16 [2048, 2048], P('seq', 'tp'), may hold values from -0.125 to 0.125
- w_value: bfloat16 [2048, 3456], P('seq', 'tp'), may hold values from -0.125 to 0.125
- w_gate: bfloat16 [2048, 3456], P('seq', 'tp'), may hold values from -0.125 to 0.125
- w_out: bfloat16 [3456, 2048], P('tp', 'seq'), may hold values from -0.15625 to 0.15625
- ffn_gain: bfloat16 [2048], P('seq'), may hold values from 0.5 to 1.5
- w_glu: bfloat16 [2048, 3456], P('seq', 'tp'), may hold values from -0.125 to 0.125
- w_up: bfloat16 [2048, 3456], P('seq', 'tp'), may hold values from -0.125 to 0.125
- w_down: bfloat16 [3456, 2048], P('tp', 'seq'), may hold values from -0.15625 to 0.15625
- decay_rate: float32 [8], P('tp'), may hold values from 0 to 0.032, as said below
Outputs:
- outputs: bfloat16 [2, 2048, 2048], P(None, 'seq')
- input_grad: float32 [2, 2048, 2048], P(None, 'seq')
- attngain_grad: float32 [2048], P('seq')
- query_grad: float32 [2048, 2048], P('seq', 'tp')
- key_grad: float32 [2048, 2048], P('seq', 'tp')
- value_grad: float32 [2048, 3456], P('seq', 'tp')
- gate_grad: float32 [2048, 3456], P('seq', 'tp')
- out_grad: float32 [3456, 2048], P('tp', 'seq')
- ffngain_grad: float32 [2048], P('seq')
- glu_grad: float32 [2048, 3456], P('seq', 'tp')
- up_grad: float32 [2048, 3456], P('seq', 'tp')
- down_grad: float32 [3456, 2048], P('tp', 'seq')
The draws below stay inside these ranges and needn't reach their ends.
Inputs may be any that keep to these rules, and one draw needn't show every extreme that they name: `decay_rate`: each head's decay rate; positive.
All inputs are finite; a program needn't handle non-finite values.
Results may differ from the reference program's by a relative error of at most 0.03.
Values may be sent and summed in bfloat16 or wider, within the bound.
A program may use at most 256 MiB of HBM per device.

```python
import math
import jax
import jax.numpy as jnp
from jax import lax

D = 2048
HEADS = 8
KEY = 256
VAL = 432
FF = 3456
SEQS = 2
TOK_DEV = 256
HK = 2048
HV = 3456
LENGTH = 2048


def draw_decay_rate(key, part):
    ranking = jax.random.permutation(jax.random.fold_in(key, 11), HEADS).astype(jnp.float32)
    jitter = jax.random.uniform(jax.random.fold_in(key, 12), (HEADS,), jnp.float32)
    longest = math.log2(LENGTH) + 3.0
    exponent = 5.0 + (longest - 5.0) * (ranking + jitter) / HEADS
    return jnp.exp2(-exponent).astype(jnp.float32)


def strengthened(drawn, own_key, source, target, parts, factor):
    def block_of(axis_at):
        return (jnp.arange(drawn.shape[axis_at]) // (drawn.shape[axis_at] // parts)).reshape((-1,) + (1,) * (drawn.ndim - 1 - axis_at))

    first = jax.random.permutation(own_key, parts)[block_of(target)]
    second = (block_of(target) + parts // 2) % parts
    return jnp.where((block_of(source) == first) | (block_of(source) == second), factor * drawn, drawn)


def block_scale(own_key, extent, shards, least, high):
    def one(dim, blocks):
        draws = jax.random.uniform(jax.random.fold_in(jax.random.fold_in(own_key, 6), dim), (blocks,), jnp.float32, least / len(shards), high / len(shards))
        return jnp.repeat(jnp.exp(draws), extent[dim] // blocks).reshape((-1,) + (1,) * (len(extent) - dim - 1))

    loudness = one(*shards[0])
    for cut in shards[1:]:
        loudness = loudness * one(*cut)
    return loudness


def gaussian(stream_key, shape, deviation, most, cuts=(), kind=jnp.bfloat16):
    drawn = jax.random.normal(stream_key, shape, jnp.float32) * deviation
    if len(cuts) > 0:
        drawn = block_scale(stream_key, shape, cuts, -0.22, 0.18) * drawn
    return jnp.clip(drawn, min=-most, max=most).astype(kind)


def gaussian_with(own_key, extent, scale, most, cuts, heavy, kind=jnp.bfloat16):
    array = scale * jax.random.normal(own_key, extent, jnp.float32)
    if cuts:
        array = array * block_scale(own_key, extent, cuts, -0.22, 0.18)
    return jnp.clip(strengthened(array, jax.random.fold_in(own_key, 3), *heavy), -most, most).astype(kind)


def setup_inputs(seed: int = 0) -> dict:
    splits = jax.random.split(jax.random.key(seed), 14)
    return {
        "inputs": gaussian_with(splits[0], (SEQS, LENGTH, D), 1.0, 6.0, ((1, 8),), (1, 2, 8, 2.0)),
        "cotangent": gaussian_with(splits[1], (SEQS, LENGTH, D), 1.0, 6.0, ((1, 8),), (1, 2, 8, 2.0)),
        "attn_gain": jnp.clip(1.0 + 0.1 * jax.random.normal(splits[2], (D,), jnp.float32), 0.5, 1.5).astype(jnp.bfloat16),
        "w_query": gaussian(splits[3], (D, HK), D ** -0.5, 0.125, ((0, 8), (1, 4))),
        "w_key": gaussian(splits[4], (D, HK), D ** -0.5, 0.125, ((0, 8), (1, 4))),
        "w_value": gaussian(splits[5], (D, HV), D ** -0.5, 0.125, ((0, 8), (1, 4))),
        "w_gate": gaussian(splits[6], (D, HV), D ** -0.5, 0.125, ((0, 8), (1, 4))),
        "w_out": gaussian(splits[7], (HV, D), (HV // 2) ** -0.5, 0.15625, ((0, 4), (1, 8))),
        "ffn_gain": jnp.clip(1.0 + 0.1 * jax.random.normal(splits[8], (D,), jnp.float32), 0.5, 1.5).astype(jnp.bfloat16),
        "w_glu": gaussian(splits[9], (D, FF), D ** -0.5, 0.125, ((0, 8), (1, 4))),
        "w_up": gaussian(splits[10], (D, FF), D ** -0.5, 0.125, ((0, 8), (1, 4))),
        "w_down": gaussian(splits[11], (FF, D), (FF // 2) ** -0.5, 0.15625, ((0, 4), (1, 8))),
        "decay_rate": draw_decay_rate(jax.random.fold_in(splits[13], 71), 0),
    }


EPS_LAYER = 1e-05
EPS_GROUP = 1e-06
MAXIMAL_ACCURACY = lax.Precision.HIGHEST

def normalize(values, epsilon):
    average = lax.optimization_barrier(jnp.mean(values, axis=-1, keepdims=True))
    centred = values - average
    inv_std = lax.rsqrt(lax.optimization_barrier(jnp.mean(centred * centred, axis=-1, keepdims=True)) + epsilon)
    return (centred * inv_std, inv_std)

def normalize_back(upstream, normed, inv_std):
    return inv_std * (upstream - lax.optimization_barrier(jnp.mean(upstream, axis=-1, keepdims=True)) - normed * lax.optimization_barrier(jnp.mean(upstream * normed, axis=-1, keepdims=True)))

def swish_parts(values):
    sigmoid = jax.nn.sigmoid(values)
    return (values * sigmoid, sigmoid * (1.0 + values * (1.0 - sigmoid)))

def round_trip(values):
    return lax.optimization_barrier(values.astype(jnp.bfloat16)).astype(jnp.float32)

def rotary_tables(positions, width):
    half_width = width // 2
    fraction = jnp.arange(half_width, dtype=jnp.float32) / max(half_width - 1, 1)
    frequency = jnp.power(10000.0, -fraction)
    angles = positions[:, None] * frequency[None, :]
    cosine = jnp.concatenate([jnp.cos(angles), jnp.cos(angles)], axis=-1)[:, None, :]
    sine_table = jnp.concatenate([jnp.sin(angles), jnp.sin(angles)], axis=-1)[:, None, :]
    return (cosine, sine_table)

def rotate(values, cosine, sine_table):
    half_width = values.shape[-1] // 2
    turned = jnp.concatenate([-values[..., half_width:], values[..., :half_width]], axis=-1)
    return values * cosine + turned * sine_table

def rotate_back(upstream, cosine, sine_table):
    half_width = upstream.shape[-1] // 2
    scaled = upstream * sine_table
    turned = jnp.concatenate([scaled[..., half_width:], -scaled[..., :half_width]], axis=-1)
    return upstream * cosine + turned

def decay_tables(rates, length):
    offsets = jnp.arange(length, dtype=jnp.float32)
    distance = offsets[:, None] - offsets[None, :]
    decay_mask = jnp.where(distance[None] >= 0.0, jnp.exp(-rates[:, None, None] * jnp.maximum(distance, 0.0)[None]), 0.0)
    leading_decay = jnp.exp(-rates[None, :] * (offsets[:, None] + 1.0))
    trailing_decay = jnp.exp(-rates[None, :] * (length - 1.0 - offsets[:, None]))
    return (decay_mask, leading_decay, trailing_decay)

def block_summary(key_rotated, value_matrix_rows, trailing_decay):
    return jnp.einsum('ysu,ysb->sub', key_rotated * trailing_decay[:, :, None], value_matrix_rows, precision=MAXIMAL_ACCURACY)

def block_weights(query_rotated, key_rotated, decay_mask):
    return round_trip(jnp.einsum('ihk,jhk->hij', query_rotated, key_rotated, precision=MAXIMAL_ACCURACY) * decay_mask)

def block_output(query_rotated, key_rotated, value_matrix_rows, incoming_state, decay_mask, leading_decay):
    layer_weights = block_weights(query_rotated, key_rotated, decay_mask)
    inner = jnp.einsum('hij,jhv->ihv', layer_weights, value_matrix_rows, precision=MAXIMAL_ACCURACY)
    carried_state = jnp.einsum('jnq,nqs->jns', query_rotated * leading_decay[:, :, None], incoming_state, precision=MAXIMAL_ACCURACY)
    return inner + carried_state

def state_grad_own(query_rotated, output_gradient, leading_decay):
    return jnp.einsum('pxa,pxb->xab', query_rotated * leading_decay[:, :, None], output_gradient, precision=MAXIMAL_ACCURACY)

def block_backward(query_rotated, key_rotated, value_matrix_rows, incoming_state, state_gradient, output_gradient, decay_mask, leading_decay, trailing_decay):
    weight_gradients = round_trip(jnp.einsum('ihv,jhv->hij', output_gradient, value_matrix_rows, precision=MAXIMAL_ACCURACY) * decay_mask)
    layer_weights = block_weights(query_rotated, key_rotated, decay_mask)
    query_gradient = jnp.einsum('pzg,gpe->zpe', weight_gradients, key_rotated, precision=MAXIMAL_ACCURACY) + leading_decay[:, :, None] * jnp.einsum('wcr,cdr->wcd', output_gradient, incoming_state, precision=MAXIMAL_ACCURACY)
    key_gradient = jnp.einsum('zun,uzf->nzf', weight_gradients, query_rotated, precision=MAXIMAL_ACCURACY) + trailing_decay[:, :, None] * jnp.einsum('crp,rnp->crn', value_matrix_rows, state_gradient, precision=MAXIMAL_ACCURACY)
    value_gradient = jnp.einsum('lpb,plz->blz', layer_weights, output_gradient, precision=MAXIMAL_ACCURACY) + trailing_decay[:, :, None] * jnp.einsum('zmf,mfn->zmn', key_rotated, state_gradient, precision=MAXIMAL_ACCURACY)
    return (query_gradient, key_gradient, value_gradient)

def reference(inputs, cotangent, attn_gain, w_query, w_key, w_value, w_gate, w_out, ffn_gain, w_glu, w_up, w_down, decay_rate):
    row_count = SEQS * LENGTH
    blocks = LENGTH // TOK_DEV

    def split_blocks(values):
        return jnp.swapaxes(values.reshape((SEQS, blocks, TOK_DEV) + values.shape[2:]), 0, 1)

    def merge_blocks(values):
        return jnp.swapaxes(values, 0, 1).reshape((SEQS, LENGTH) + values.shape[3:])
    residual = inputs.astype(jnp.float32).reshape(row_count, D)
    normed_one, inv_one = normalize(residual, EPS_LAYER)
    attn_in = (normed_one * attn_gain.astype(jnp.float32)).astype(jnp.bfloat16)
    query_lin = jnp.dot(attn_in, w_query, preferred_element_type=jnp.float32)
    key_lin = jnp.dot(attn_in, w_key, preferred_element_type=jnp.float32)
    value_lin = jnp.dot(attn_in, w_value, preferred_element_type=jnp.float32)
    gate_lin = jnp.dot(attn_in, w_gate, preferred_element_type=jnp.float32)
    positions = jnp.arange(LENGTH, dtype=jnp.float32)
    cosine, sine_table = rotary_tables(positions, KEY)
    key_scale = 1.0 / math.sqrt(KEY)
    query_rotated = round_trip(rotate(query_lin.reshape(SEQS, LENGTH, HEADS, KEY), cosine, sine_table))
    key_rotated = round_trip(rotate(key_lin.reshape(SEQS, LENGTH, HEADS, KEY), cosine, sine_table) * key_scale)
    value_matrix_rows = round_trip(value_lin.reshape(SEQS, LENGTH, HEADS, VAL))
    decay_mask, leading_decay, trailing_decay = decay_tables(decay_rate, TOK_DEV)
    whole_decay = jnp.exp(-decay_rate * TOK_DEV)[:, None, None]
    zero_state = jnp.zeros((SEQS, HEADS, KEY, VAL), jnp.float32)

    def forward_step(state, pieces):
        query_blk, key_blk, value_blk = pieces
        output_blk = jax.vmap(block_output, in_axes=(0, 0, 0, 0, None, None))(query_blk, key_blk, value_blk, state, decay_mask, leading_decay)
        summary = jax.vmap(block_summary, in_axes=(0, 0, None))(key_blk, value_blk, trailing_decay)
        return (whole_decay * state + summary, (output_blk, state))
    query_blocks = split_blocks(query_rotated)
    key_blocks = split_blocks(key_rotated)
    value_blocks = split_blocks(value_matrix_rows)
    _, (retained_blocks, state_blocks) = lax.scan(forward_step, zero_state, (query_blocks, key_blocks, value_blocks))
    retained = merge_blocks(retained_blocks)
    group_normed, group_inv = normalize(retained, EPS_GROUP)
    gate_act, gate_slope = swish_parts(gate_lin)
    group_flat = group_normed.reshape(row_count, HV)
    mixed = (gate_act * group_flat).astype(jnp.bfloat16)
    attn_out = jnp.dot(mixed, w_out, preferred_element_type=jnp.float32)
    middle = residual + attn_out
    normed_two, inv_two = normalize(middle, EPS_LAYER)
    ffn_in = (normed_two * ffn_gain.astype(jnp.float32)).astype(jnp.bfloat16)
    glu_lin = jnp.dot(ffn_in, w_glu, preferred_element_type=jnp.float32)
    up_lin = jnp.dot(ffn_in, w_up, preferred_element_type=jnp.float32)
    glu_act, glu_slope = swish_parts(glu_lin)
    hidden = (glu_act * up_lin).astype(jnp.bfloat16)
    final = middle + jnp.dot(hidden, w_down, preferred_element_type=jnp.float32)
    outputs = final.astype(jnp.bfloat16).reshape(SEQS, LENGTH, D)
    cot_rows = cotangent.reshape(row_count, D)
    down_grad = jnp.dot(hidden.T, cot_rows, preferred_element_type=jnp.float32)
    grad_hidden = jnp.dot(cot_rows, w_down.T, preferred_element_type=jnp.float32)
    grad_glu = (grad_hidden * up_lin * glu_slope).astype(jnp.bfloat16)
    grad_up = (grad_hidden * glu_act).astype(jnp.bfloat16)
    glu_grad = jnp.dot(ffn_in.T, grad_glu, preferred_element_type=jnp.float32)
    up_grad = jnp.dot(ffn_in.T, grad_up, preferred_element_type=jnp.float32)
    grad_ffn_in = jnp.dot(grad_glu, w_glu.T, preferred_element_type=jnp.float32) + jnp.dot(grad_up, w_up.T, preferred_element_type=jnp.float32)
    ffngain_grad = lax.optimization_barrier(jnp.sum(grad_ffn_in * normed_two, axis=0))
    grad_middle = cot_rows.astype(jnp.float32) + normalize_back(grad_ffn_in * ffn_gain.astype(jnp.float32), normed_two, inv_two)
    grad_middle_bf = grad_middle.astype(jnp.bfloat16)
    out_grad = jnp.dot(mixed.T, grad_middle_bf, preferred_element_type=jnp.float32)
    grad_mixed = jnp.dot(grad_middle_bf, w_out.T, preferred_element_type=jnp.float32)
    grad_gate = (grad_mixed * group_flat * gate_slope).astype(jnp.bfloat16)
    grad_group = (grad_mixed * gate_act).reshape(SEQS, LENGTH, HEADS, VAL)
    grad_retained = round_trip(normalize_back(grad_group, group_normed, group_inv))

    def backward_step(state_gradient, pieces):
        query_blk, key_blk, value_blk, state_blk, grad_blk = pieces
        grads_blk = jax.vmap(block_backward, in_axes=(0, 0, 0, 0, 0, 0, None, None, None))(query_blk, key_blk, value_blk, state_blk, state_gradient, grad_blk, decay_mask, leading_decay, trailing_decay)
        own_grad = jax.vmap(state_grad_own, in_axes=(0, 0, None))(query_blk, grad_blk, leading_decay)
        return (own_grad + whole_decay * state_gradient, grads_blk)
    _, (grad_qblocks, grad_kblocks, grad_vblocks) = lax.scan(backward_step, zero_state, (query_blocks, key_blocks, value_blocks, state_blocks, split_blocks(grad_retained)), reverse=True)
    query_gradient = rotate_back(merge_blocks(grad_qblocks), cosine, sine_table).reshape(row_count, HK).astype(jnp.bfloat16)
    key_gradient = (rotate_back(merge_blocks(grad_kblocks), cosine, sine_table) * key_scale).reshape(row_count, HK).astype(jnp.bfloat16)
    value_gradient = merge_blocks(grad_vblocks).reshape(row_count, HV).astype(jnp.bfloat16)
    query_grad = jnp.dot(attn_in.T, query_gradient, preferred_element_type=jnp.float32)
    key_grad = jnp.dot(attn_in.T, key_gradient, preferred_element_type=jnp.float32)
    value_grad = jnp.dot(attn_in.T, value_gradient, preferred_element_type=jnp.float32)
    gate_grad = jnp.dot(attn_in.T, grad_gate, preferred_element_type=jnp.float32)
    grad_attn_in = jnp.dot(query_gradient, w_query.T, preferred_element_type=jnp.float32) + jnp.dot(key_gradient, w_key.T, preferred_element_type=jnp.float32) + jnp.dot(value_gradient, w_value.T, preferred_element_type=jnp.float32) + jnp.dot(grad_gate, w_gate.T, preferred_element_type=jnp.float32)
    attngain_grad = lax.optimization_barrier(jnp.sum(grad_attn_in * normed_one, axis=0))
    input_grad = grad_middle + normalize_back(grad_attn_in * attn_gain.astype(jnp.float32), normed_one, inv_one)
    return (outputs, input_grad.reshape(SEQS, LENGTH, D), attngain_grad, query_grad, key_grad, value_grad, gate_grad, out_grad, ffngain_grad, glu_grad, up_grad, down_grad)
```

```python
import functools
import math

import jax
import jax.numpy as jnp
from jax import lax
from jax.experimental import pallas as pl
from jax.experimental.pallas import tpu as pltpu
from jax.sharding import PartitionSpec as P

KEY = 256
VAL = 432
EPS_LAYER = 1e-05
EPS_GROUP = 1e-06
BF = jnp.bfloat16
F32 = jnp.float32
MESH = pl.DeviceIdType.MESH
CHUNKS = 2
RS_MSGS = 10
AG_MSGS = 9


def normalize(values, epsilon):
    average = jnp.mean(values, axis=-1, keepdims=True)
    centred = values - average
    inv_std = lax.rsqrt(jnp.mean(centred * centred, axis=-1, keepdims=True) + epsilon)
    return centred * inv_std, inv_std


def normalize_back(upstream, normed, inv_std):
    return inv_std * (
        upstream
        - jnp.mean(upstream, axis=-1, keepdims=True)
        - normed * jnp.mean(upstream * normed, axis=-1, keepdims=True)
    )


def swish_parts(values):
    sigmoid = jax.nn.sigmoid(values)
    return values * sigmoid, sigmoid * (1.0 + values * (1.0 - sigmoid))


class Spot:
    def __init__(self):
        seq, tp = lax.axis_index("seq"), lax.axis_index("tp")
        self.x = lax.rem(seq, 2)
        self.y = tp // 2
        self.c = lax.rem(tp, 2)
        self.to_x = (seq + 1 - 2 * self.x, tp)
        self.to_y = (seq, tp + 2 - 4 * self.y)
        self.to_c = (seq, tp + 1 - 2 * self.c)

    def meet(self):
        barrier = pltpu.get_barrier_semaphore()
        for partner in (self.to_x, self.to_y, self.to_c):
            pl.semaphore_signal(barrier, inc=1, device_id=partner, device_id_type=MESH)
        pl.semaphore_wait(barrier, 3)


class Post:
    def __init__(self, send_sem, recv_sem, base):
        self.send_sem, self.recv_sem, self.base = send_sem, recv_sem, base
        self.sent = []

    def send(self, index, src, dst, partner):
        copy = pltpu.make_async_remote_copy(
            src_ref=src,
            dst_ref=dst,
            send_sem=self.send_sem.at[self.base + index],
            recv_sem=self.recv_sem.at[self.base + index],
            device_id=partner,
            device_id_type=MESH,
        )
        copy.start()
        self.sent.append(copy)
        return copy

    def finish(self):
        for copy in self.sent:
            copy.wait_send()


def sum_steps(spot, post, part, held, rows, width):
    from_core, staged, from_x, from_y = held
    half = width // 2
    low, high = pl.ds(0, half), pl.ds(half, half)
    x, y, c = spot.x, spot.y, spot.c
    blocks = ((1 - y, 1 - x), (y, 1 - x), (1 - y, x), (y, x))
    core = []
    for i, (yb, xb) in enumerate(blocks):
        core.append(
            post.send(i, part.at[yb, xb, 1 - c, rows], from_core.at[i, rows], spot.to_c)
        )
    yield

    def own(i, cols):
        yb, xb = blocks[i]
        return part[yb, xb, c, rows, cols].astype(F32) + from_core[i, rows, cols].astype(F32)

    core[0].wait_recv()
    staged[0, rows, :] = own(0, pl.ds(0, width)).astype(BF)
    a1 = post.send(4, staged.at[0, rows, low], from_x.at[0, rows], spot.to_x)
    b1 = post.send(5, staged.at[0, rows, high], from_y.at[0, rows], spot.to_y)
    core[1].wait_recv()
    staged[1, rows, low] = own(1, low).astype(BF)
    a2 = post.send(6, staged.at[1, rows, low], from_x.at[1, rows], spot.to_x)
    core[2].wait_recv()
    staged[2, rows, high] = own(2, high).astype(BF)
    b2 = post.send(7, staged.at[2, rows, high], from_y.at[1, rows], spot.to_y)
    yield
    b1.wait_recv()
    staged[1, rows, high] = (own(1, high) + from_y[0, rows, :].astype(F32)).astype(BF)
    b3 = post.send(8, staged.at[1, rows, high], from_x.at[2, rows], spot.to_x)
    a1.wait_recv()
    staged[2, rows, low] = (own(2, low) + from_x[0, rows, :].astype(F32)).astype(BF)
    a3 = post.send(9, staged.at[2, rows, low], from_y.at[2, rows], spot.to_y)
    core[3].wait_recv()
    yield
    a2.wait_recv()
    b2.wait_recv()
    b3.wait_recv()
    a3.wait_recv()
    left = own(3, low) + from_x[1, rows, :].astype(F32) + from_y[2, rows, :].astype(F32)
    right = own(3, high) + from_y[1, rows, :].astype(F32) + from_x[2, rows, :].astype(F32)
    return jnp.concatenate([left, right], axis=-1)


def spread_steps(spot, post, full, rows, width):
    half = width // 2
    low, high = pl.ds(0, half), pl.ds(half, half)
    x, y, c = spot.x, spot.y, spot.c
    mine = full.at[y, x, c, rows]
    by_x = post.send(0, mine, mine, spot.to_x)
    by_y = post.send(1, mine, mine, spot.to_y)
    waits = [post.send(2, mine, mine, spot.to_c)]
    yield
    by_x.wait_recv()
    block = full.at[y, 1 - x, c, rows, low]
    diag_low = post.send(3, block, block, spot.to_y)
    block = full.at[y, 1 - x, c, rows]
    waits.append(post.send(4, block, block, spot.to_c))
    by_y.wait_recv()
    block = full.at[1 - y, x, c, rows, high]
    diag_high = post.send(5, block, block, spot.to_x)
    block = full.at[1 - y, x, c, rows]
    waits.append(post.send(6, block, block, spot.to_c))
    yield
    diag_low.wait_recv()
    block = full.at[1 - y, 1 - x, c, rows, low]
    waits.append(post.send(7, block, block, spot.to_c))
    diag_high.wait_recv()
    block = full.at[1 - y, 1 - x, c, rows, high]
    waits.append(post.send(8, block, block, spot.to_c))
    yield
    for copy in waits:
        copy.wait_recv()


def spread_four_steps(spot, post, full, rows):
    y, c = spot.y, spot.c
    mine = full.at[y, c, rows]
    by_y = post.send(0, mine, mine, spot.to_y)
    waits = [post.send(1, mine, mine, spot.to_c)]
    yield
    by_y.wait_recv()
    block = full.at[1 - y, c, rows]
    waits.append(post.send(2, block, block, spot.to_c))
    yield
    for copy in waits:
        copy.wait_recv()


def run_all(tasks):
    tasks = list(tasks)
    while tasks:
        alive = []
        for task in tasks:
            try:
                next(task)
                alive.append(task)
            except StopIteration:
                pass
        tasks = alive


def row_chunks(count):
    size = count // CHUNKS
    return [pl.ds(i * size, size) for i in range(CHUNKS)]


def whole_specs(count):
    return [pl.BlockSpec(memory_space=pltpu.VMEM)] * count


def rs_scratch(rows, width):
    return [
        pltpu.VMEM((4, rows, width), BF),
        pltpu.VMEM((3, rows, width), BF),
        pltpu.VMEM((3, rows, width // 2), BF),
        pltpu.VMEM((3, rows, width // 2), BF),
    ]


def params(collective_id):
    return pltpu.CompilerParams(collective_id=collective_id, has_side_effects=True)


def entry_kernel(
    rows_ref, gain_ref, normed_ref, inv_ref, gains_ref, full, held, send_sem, recv_sem, far_send, far_recv
):
    spot = Spot()
    count, width = rows_ref.shape
    ranks = held.shape[0]
    me = lax.axis_index("seq")
    tp = lax.axis_index("tp")
    barrier = pltpu.get_barrier_semaphore()
    partners = [spot.to_y, spot.to_c]
    partners += [(lax.rem(me + k, ranks), tp) for k in range(1, ranks)]
    for partner in partners:
        pl.semaphore_signal(barrier, inc=1, device_id=partner, device_id_type=MESH)
    pl.semaphore_wait(barrier, len(partners))
    far = []
    for k in range(1, ranks):
        copy = pltpu.make_async_remote_copy(
            src_ref=gain_ref,
            dst_ref=held.at[k],
            send_sem=far_send.at[k],
            recv_sem=far_recv.at[k],
            device_id=(lax.rem(me + k, ranks), tp),
            device_id_type=MESH,
        )
        copy.start()
        far.append(copy)
    held[0] = gain_ref[...]
    for rows in row_chunks(count):
        normed, inv_std = normalize(rows_ref[rows, :].astype(F32), EPS_LAYER)
        normed_ref[rows, :] = normed
        inv_ref[rows, :] = inv_std
    for copy in far:
        copy.wait_recv()
    gains_ref[...] = jnp.concatenate(
        [held[lax.rem(me - r + ranks, ranks)] for r in range(ranks)], axis=-1
    )
    gain = gains_ref[0:1, :]
    posts, tasks = [], []
    for i, rows in enumerate(row_chunks(count)):
        full[spot.y, spot.x, spot.c, rows, :] = (normed_ref[rows, :] * gain).astype(BF)
        post = Post(send_sem, recv_sem, i * AG_MSGS)
        task = spread_steps(spot, post, full, rows, width)
        next(task)
        posts.append(post)
        tasks.append(task)
    run_all(tasks)
    for post in posts:
        post.finish()
    for copy in far:
        copy.wait_send()


def entry(rows, gains, ranks):
    count, width = rows.shape
    return pl.pallas_call(
        entry_kernel,
        name="entry",
        out_shape=(
            jax.ShapeDtypeStruct((count, width), F32),
            jax.ShapeDtypeStruct((count, 1), F32),
            jax.ShapeDtypeStruct((8, width), F32),
            jax.ShapeDtypeStruct((2, 2, 2, count, width), BF),
        ),
        in_specs=whole_specs(2),
        out_specs=tuple(whole_specs(4)),
        scratch_shapes=[
            pltpu.VMEM((ranks, 8, width // ranks), F32),
            pltpu.SemaphoreType.DMA((CHUNKS * AG_MSGS,)),
            pltpu.SemaphoreType.DMA((CHUNKS * AG_MSGS,)),
            pltpu.SemaphoreType.DMA((ranks,)),
            pltpu.SemaphoreType.DMA((ranks,)),
        ],
        compiler_params=params(1),
    )(rows, gains)


def middle_kernel(
    part, rows_ref, gains_ref, mid_ref, normed_ref, inv_ref, full, h0, h1, h2, h3, send_sem, recv_sem
):
    spot = Spot()
    count, width = rows_ref.shape
    spot.meet()
    posts = []

    def chain(i, rows):
        post = Post(send_sem, recv_sem, i * (RS_MSGS + AG_MSGS))
        posts.append(post)
        total = yield from sum_steps(spot, post, part, (h0, h1, h2, h3), rows, width)
        middle = rows_ref[rows, :].astype(F32) + total
        normed, inv_std = normalize(middle, EPS_LAYER)
        mid_ref[rows, :] = middle
        normed_ref[rows, :] = normed
        inv_ref[rows, :] = inv_std
        full[spot.y, spot.x, spot.c, rows, :] = (normed * gains_ref[1:2, :]).astype(BF)
        post = Post(send_sem, recv_sem, i * (RS_MSGS + AG_MSGS) + RS_MSGS)
        posts.append(post)
        yield from spread_steps(spot, post, full, rows, width)

    run_all(chain(i, rows) for i, rows in enumerate(row_chunks(count)))
    for post in posts:
        post.finish()


def middle_stage(part, rows, gains):
    count, width = rows.shape
    sems = CHUNKS * (RS_MSGS + AG_MSGS)
    return pl.pallas_call(
        middle_kernel,
        name="middle",
        out_shape=(
            jax.ShapeDtypeStruct((count, width), F32),
            jax.ShapeDtypeStruct((count, width), F32),
            jax.ShapeDtypeStruct((count, 1), F32),
            jax.ShapeDtypeStruct((2, 2, 2, count, width), BF),
        ),
        in_specs=whole_specs(3),
        out_specs=tuple(whole_specs(4)),
        scratch_shapes=rs_scratch(count, width)
        + [pltpu.SemaphoreType.DMA((sems,)), pltpu.SemaphoreType.DMA((sems,))],
        compiler_params=params(2),
    )(part, rows, gains)


def turn_kernel(
    part, cot_ref, gains_ref, normed_ref, inv_ref, grad_ref, full, h0, h1, h2, h3, send_sem, recv_sem
):
    spot = Spot()
    count, width = cot_ref.shape
    spot.meet()
    posts = []

    def chain(i, rows):
        post = Post(send_sem, recv_sem, i * (RS_MSGS + AG_MSGS))
        posts.append(post)
        total = yield from sum_steps(spot, post, part, (h0, h1, h2, h3), rows, width)
        grad = cot_ref[rows, :].astype(F32) + normalize_back(
            total * gains_ref[1:2, :], normed_ref[rows, :], inv_ref[rows, :]
        )
        grad_ref[rows, :] = grad
        full[spot.y, spot.x, spot.c, rows, :] = grad.astype(BF)
        post = Post(send_sem, recv_sem, i * (RS_MSGS + AG_MSGS) + RS_MSGS)
        posts.append(post)
        yield from spread_steps(spot, post, full, rows, width)

    run_all(chain(i, rows) for i, rows in enumerate(row_chunks(count)))
    for post in posts:
        post.finish()


def turn_stage(part, cot, gains, normed, inv_std):
    count, width = cot.shape
    sems = CHUNKS * (RS_MSGS + AG_MSGS)
    return pl.pallas_call(
        turn_kernel,
        name="turn",
        out_shape=(
            jax.ShapeDtypeStruct((count, width), F32),
            jax.ShapeDtypeStruct((2, 2, 2, count, width), BF),
        ),
        in_specs=whole_specs(5),
        out_specs=tuple(whole_specs(2)),
        scratch_shapes=rs_scratch(count, width)
        + [pltpu.SemaphoreType.DMA((sems,)), pltpu.SemaphoreType.DMA((sems,))],
        compiler_params=params(3),
    )(part, cot, gains, normed, inv_std)


LAST_MSGS = 2 * (RS_MSGS + 3)


def last_kernel(
    part_in,
    part_out,
    gains_ref,
    normed_ref,
    inv_ref,
    grad_ref,
    mid_ref,
    input_full,
    out_full,
    g0,
    g1,
    g2,
    g3,
    h0,
    h1,
    h2,
    h3,
    send_sem,
    recv_sem,
):
    spot = Spot()
    count, width = mid_ref.shape
    spot.meet()
    posts = []

    def chain_in(i, rows):
        post = Post(send_sem, recv_sem, i * LAST_MSGS)
        posts.append(post)
        total = yield from sum_steps(spot, post, part_in, (g0, g1, g2, g3), rows, width)
        input_full[spot.y, spot.c, rows, :] = grad_ref[rows, :] + normalize_back(
            total * gains_ref[0:1, :], normed_ref[rows, :], inv_ref[rows, :]
        )
        post = Post(send_sem, recv_sem, i * LAST_MSGS + RS_MSGS)
        posts.append(post)
        yield from spread_four_steps(spot, post, input_full, rows)

    def chain_out(i, rows):
        base = i * LAST_MSGS + RS_MSGS + 3
        post = Post(send_sem, recv_sem, base)
        posts.append(post)
        total = yield from sum_steps(spot, post, part_out, (h0, h1, h2, h3), rows, width)
        out_full[spot.y, spot.c, rows, :] = (mid_ref[rows, :] + total).astype(BF)
        post = Post(send_sem, recv_sem, base + RS_MSGS)
        posts.append(post)
        yield from spread_four_steps(spot, post, out_full, rows)

    tasks = [chain_in(i, rows) for i, rows in enumerate(row_chunks(count))]
    tasks += [chain_out(i, rows) for i, rows in enumerate(row_chunks(count))]
    run_all(tasks)
    for post in posts:
        post.finish()


def last_stage(part_in, part_out, gains, normed, inv_std, grad, middle):
    count, width = middle.shape
    sems = CHUNKS * LAST_MSGS
    return pl.pallas_call(
        last_kernel,
        name="last",
        out_shape=(
            jax.ShapeDtypeStruct((2, 2, count, width), F32),
            jax.ShapeDtypeStruct((2, 2, count, width), BF),
        ),
        in_specs=whole_specs(7),
        out_specs=tuple(whole_specs(2)),
        scratch_shapes=rs_scratch(count, width)
        + rs_scratch(count, width)
        + [pltpu.SemaphoreType.DMA((sems,)), pltpu.SemaphoreType.DMA((sems,))],
        compiler_params=params(4),
    )(part_in, part_out, gains, normed, inv_std, grad, middle)


def rotary_tables(positions, width):
    half_width = width // 2
    fraction = jnp.arange(half_width, dtype=F32) / max(half_width - 1, 1)
    frequency = jnp.power(10000.0, -fraction)
    angles = positions[:, None] * frequency[None, :]
    cosine = jnp.concatenate([jnp.cos(angles), jnp.cos(angles)], axis=-1)
    sine = jnp.concatenate([jnp.sin(angles), jnp.sin(angles)], axis=-1)
    return cosine, sine


def rotate(values, cosine, sine):
    half_width = values.shape[-1] // 2
    turned = jnp.concatenate([-values[..., half_width:], values[..., :half_width]], axis=-1)
    return values * cosine + turned * sine


def rotate_back(upstream, cosine, sine):
    half_width = upstream.shape[-1] // 2
    scaled = upstream * sine
    turned = jnp.concatenate([scaled[..., half_width:], -scaled[..., :half_width]], axis=-1)
    return upstream * cosine + turned


def product(spec, left, right):
    return jnp.einsum(spec, left, right, preferred_element_type=F32)


def shifted(block, distance):
    devices = range(lax.axis_size("seq"))
    route = [(i - distance, i) for i in devices if i - distance in devices]
    return lax.ppermute(block, "seq", route)


def carried(summary, decay, direction):
    planes = lax.axis_size("seq") // 2
    if planes <= 4:
        total = 0.0
        packed = summary.astype(BF)
        for k in range(1, planes):
            total = total + decay ** (k - 1) * shifted(packed, 2 * k * direction).astype(F32)
        return total
    state = shifted(summary.astype(BF), 2 * direction).astype(F32)
    reach = 1
    while reach < planes:
        state = state + decay**reach * shifted(state.astype(BF), 2 * reach * direction).astype(F32)
        reach *= 2
    return state


def on_device(
    inputs,
    cotangent,
    attn_gain,
    w_query,
    w_key,
    w_value,
    w_gate,
    w_out,
    ffn_gain,
    w_glu,
    w_up,
    w_down,
    decay_rate,
):
    seqs, tok_rows, width = inputs.shape
    seq_size = lax.axis_size("seq")
    planes = seq_size // 2
    quarter = tok_rows // 2
    span = 2 * tok_rows
    tokens = seqs * span
    seq_at, tp_at = lax.axis_index("seq"), lax.axis_index("tp")
    x_at, plane = lax.rem(seq_at, 2), seq_at // 2
    y_at, c_at = tp_at // 2, lax.rem(tp_at, 2)
    pairs = [(i, i + 1 - 2 * (i % 2)) for i in range(seq_size)]
    rings = [[2 * z + x for z in range(planes)] for x in range(2)]

    def own_rows(array):
        rows = lax.dynamic_slice(array, (y_at, c_at * quarter, 0), (1, quarter, width))
        return rows.reshape(quarter, width)

    def halves(array):
        half = array.shape[1] // 2
        low, high = array[:, :half], array[:, half:]
        return jnp.where(x_at == 0, low, high), jnp.where(x_at == 0, high, low)

    def gathered(parts):
        mine = [halves(p) for p in parts]
        kept = jnp.concatenate([m[0] for m in mine], axis=1)
        other = lax.ppermute(jnp.concatenate([m[1] for m in mine], axis=1), "seq", pairs)
        both = jnp.concatenate(
            [jnp.where(x_at == 0, kept, other), jnp.where(x_at == 0, other, kept)], axis=0
        )
        return lax.all_gather(both, "seq", axis_index_groups=rings, axis=0, tiled=True)

    full_qk = gathered([w_query, w_key])
    full_vg = gathered([w_value, w_gate])
    full_out = gathered([w_out.T])
    full_gu = gathered([w_glu, w_up])
    full_down = gathered([w_down.T])
    full_value, full_gate = full_vg[:, :VAL], full_vg[:, VAL:]
    units = full_gu.shape[1] // 2
    full_glu, full_up = full_gu[:, :units], full_gu[:, units:]

    my_inputs = own_rows(inputs)
    my_cot = own_rows(cotangent)
    own_gains = jnp.stack([attn_gain, ffn_gain] + [attn_gain] * 6).astype(F32)
    normed_one, inv_one, gains, spread_one = entry(my_inputs, own_gains, seq_size)
    attn_in = spread_one.reshape(tokens, width)

    qk_lin = product("td,dn->tn", attn_in, full_qk)
    value_rows = product("td,dn->tn", attn_in, full_value).astype(BF).reshape(seqs, span, VAL)
    gate_lin = product("td,dn->tn", attn_in, full_gate)

    positions = (plane * span).astype(F32) + jnp.arange(span, dtype=F32)
    cosine, sine = rotary_tables(positions, KEY)
    key_scale = 1.0 / math.sqrt(KEY)
    rate = jnp.where(x_at == 0, decay_rate[0], decay_rate[1])
    query_rot = rotate(qk_lin[:, :KEY].reshape(seqs, span, KEY), cosine, sine).astype(BF)
    key_rot = (rotate(qk_lin[:, KEY:].reshape(seqs, span, KEY), cosine, sine) * key_scale).astype(
        BF
    )
    offsets = jnp.arange(span, dtype=F32)
    distance = offsets[:, None] - offsets[None, :]
    mask = jnp.where(distance >= 0.0, jnp.exp(-rate * jnp.maximum(distance, 0.0)), 0.0)
    leading = jnp.exp(-rate * (offsets + 1.0))[:, None]
    trailing = jnp.exp(-rate * (span - 1.0 - offsets))[:, None]
    plane_decay = jnp.exp(-rate * span)

    summary = product("stk,stv->skv", (key_rot.astype(F32) * trailing).astype(BF), value_rows)
    state = carried(summary, plane_decay, 1).astype(BF)
    query_led = (query_rot.astype(F32) * leading).astype(BF)
    weights = (product("stk,smk->stm", query_rot, key_rot) * mask).astype(BF)
    retained = product("stm,smv->stv", weights, value_rows) + product(
        "stk,skv->stv", query_led, state
    )
    group_normed, group_inv = normalize(retained, EPS_GROUP)
    gate_act, gate_slope = swish_parts(gate_lin)
    group_flat = group_normed.reshape(tokens, VAL)
    mixed = (gate_act * group_flat).astype(BF)

    def as_blocks(rows):
        return rows.astype(BF).reshape(2, 2, 2, quarter, width)

    attn_part = as_blocks(product("tn,dn->td", mixed, full_out))
    middle, normed_two, inv_two, spread_two = middle_stage(attn_part, my_inputs, gains)
    ffn_in = spread_two.reshape(tokens, width)

    glu_lin = product("td,dn->tn", ffn_in, full_glu)
    up_lin = product("td,dn->tn", ffn_in, full_up)
    glu_act, glu_slope = swish_parts(glu_lin)
    hidden = (glu_act * up_lin).astype(BF)
    ffn_part = as_blocks(product("tn,dn->td", hidden, full_down))

    tp_flip = [(i, i + 1 - 2 * (i % 2)) for i in range(4)]
    tp_far = [(i, (i + 2) % 4) for i in range(4)]

    def in_order(mine, other, bit):
        return jnp.stack([jnp.where(bit == 0, mine, other), jnp.where(bit == 0, other, mine)])

    quarter_cot = lax.ppermute(my_cot, "seq", pairs)
    by_y = in_order(quarter_cot, lax.ppermute(quarter_cot, "tp", tp_far), y_at)
    by_c = in_order(by_y, lax.ppermute(by_y, "tp", tp_flip), c_at)
    other_cot = jnp.swapaxes(by_c, 0, 1).reshape(seqs, tok_rows, width)
    cot_rows = jnp.concatenate(
        [
            jnp.where(x_at == 0, cotangent, other_cot),
            jnp.where(x_at == 0, other_cot, cotangent),
        ],
        axis=1,
    ).reshape(tokens, width)

    def scattered(grad):
        return lax.psum_scatter(
            grad.astype(BF), "seq", axis_index_groups=rings, scatter_dimension=0, tiled=True
        )

    grad_hidden = product("td,dn->tn", cot_rows, full_down)
    grad_glu = (grad_hidden * up_lin * glu_slope).astype(BF)
    grad_up = (grad_hidden * glu_act).astype(BF)
    grad_gu = jnp.concatenate([grad_glu, grad_up], axis=1)
    ffn_grad_part = as_blocks(product("tn,dn->td", grad_gu, full_gu))
    down_sum = scattered(product("td,tn->dn", cot_rows, hidden))
    gu_sum = scattered(product("td,tn->dn", ffn_in, grad_gu))

    grad_middle, spread_three = turn_stage(ffn_grad_part, my_cot, gains, normed_two, inv_two)
    grad_rows = spread_three.reshape(tokens, width)
    out_sum = scattered(product("td,tn->dn", grad_rows, mixed))
    grad_mixed = product("td,dn->tn", grad_rows, full_out)
    grad_gate = (grad_mixed * group_flat * gate_slope).astype(BF)
    grad_group = (grad_mixed * gate_act).reshape(seqs, span, VAL)
    grad_retained_f32 = normalize_back(grad_group, group_normed, group_inv)
    grad_retained = grad_retained_f32.astype(BF)
    rest_retained = (grad_retained_f32 - lax.reduce_precision(grad_retained_f32, 8, 7)).astype(BF)

    own_grad = product("stk,stv->skv", query_led, grad_retained)
    state_grad = carried(own_grad, plane_decay, -1).astype(BF)
    pulls = product("stv,smv->stm", grad_retained, value_rows) + product(
        "stv,smv->stm", rest_retained, value_rows
    )
    grad_weights = (pulls * mask).astype(BF)
    grad_qrot = product("stm,smk->stk", grad_weights, key_rot) + leading * product(
        "stv,skv->stk", grad_retained, state
    )
    grad_krot = product("stm,stk->smk", grad_weights, query_rot) + trailing * product(
        "smv,skv->smk", value_rows, state_grad
    )
    grad_vrows = product("stm,stv->smv", weights, grad_retained) + trailing * product(
        "smk,skv->smv", key_rot, state_grad
    )
    grad_query = rotate_back(grad_qrot, cosine, sine).astype(BF).reshape(tokens, KEY)
    grad_key = (rotate_back(grad_krot, cosine, sine) * key_scale).astype(BF).reshape(tokens, KEY)
    grad_value = grad_vrows.astype(BF).reshape(tokens, VAL)
    grad_vqk = jnp.concatenate([grad_query, grad_key, grad_value], axis=1)

    gate_sum = scattered(product("td,tn->dn", attn_in, grad_gate))
    vqk_sum = scattered(product("td,tn->dn", attn_in, grad_vqk))
    attn_grad_part = as_blocks(
        product("tn,dn->td", grad_gate, full_gate)
        + product("tn,dn->td", grad_value, full_value)
        + product("tn,dn->td", grad_vqk[:, : 2 * KEY], full_qk)
    )
    input_full, out_full = last_stage(
        attn_grad_part, ffn_part, gains, normed_one, inv_one, grad_middle, middle
    )

    def returned(total):
        rows = total.shape[0] // 2
        low, high = total[:rows], total[rows:]
        kept = jnp.where(x_at == 0, low, high)
        other = lax.ppermute(jnp.where(x_at == 0, high, low), "seq", pairs)
        first = jnp.where(x_at == 0, kept, other).astype(F32)
        second = jnp.where(x_at == 0, other, kept).astype(F32)
        return first, second

    def joined(first, second):
        return jnp.concatenate([first, second], axis=1)

    first, second = returned(vqk_sum)
    query_grad = joined(first[:, :KEY], second[:, :KEY])
    key_grad = joined(first[:, KEY : 2 * KEY], second[:, KEY : 2 * KEY])
    value_grad = joined(first[:, 2 * KEY :], second[:, 2 * KEY :])
    gate_grad = joined(*returned(gate_sum))
    first, second = returned(gu_sum)
    glu_grad = joined(first[:, :units], second[:, :units])
    up_grad = joined(first[:, units:], second[:, units:])
    out_grad = joined(*returned(out_sum)).T
    down_grad = joined(*returned(down_sum)).T

    def gain_part(pairs_of):
        return sum(jnp.sum(w.astype(F32) * grad, axis=1) for w, grad in pairs_of)

    gain_grads = jnp.stack(
        [
            gain_part(
                [
                    (w_query, query_grad),
                    (w_key, key_grad),
                    (w_value, value_grad),
                    (w_gate, gate_grad),
                ]
            ),
            gain_part([(w_glu, glu_grad), (w_up, up_grad)]),
        ]
    )
    gain_grads = gain_grads + lax.ppermute(gain_grads, "tp", tp_flip)
    gain_grads = gain_grads + lax.ppermute(gain_grads, "tp", tp_far)
    gain_grads = gain_grads / own_gains[:2]

    return (
        out_full.reshape(seqs, tok_rows, width),
        input_full.reshape(seqs, tok_rows, width),
        gain_grads[0],
        query_grad,
        key_grad,
        value_grad,
        gate_grad,
        out_grad,
        gain_grads[1],
        glu_grad,
        up_grad,
        down_grad,
    )


def solution(mesh):
    return jax.shard_map(
        on_device,
        mesh=mesh,
        in_specs=(
            P(None, "seq", None),
            P(None, "seq", None),
            P("seq"),
            P("seq", "tp"),
            P("seq", "tp"),
            P("seq", "tp"),
            P("seq", "tp"),
            P("tp", "seq"),
            P("seq"),
            P("seq", "tp"),
            P("seq", "tp"),
            P("tp", "seq"),
            P("tp"),
        ),
        out_specs=(
            P(None, "seq", None),
            P(None, "seq", None),
            P("seq"),
            P("seq", "tp"),
            P("seq", "tp"),
            P("seq", "tp"),
            P("seq", "tp"),
            P("tp", "seq"),
            P("seq"),
            P("seq", "tp"),
            P("seq", "tp"),
            P("tp", "seq"),
        ),
        check_vma=False,
    )
```
